128 devices in a mesh: seq: 8 (over z_hi, x), exp: 16 (over z_lo, y, core).
Axes of the slice: x: 4, y: 4, z: 4 (z_hi: 2, z_lo: 2; z = z_hi * 2 + z_lo), core: 2. Of those that a mesh axis runs over, the one named last changes fastest.
Arguments:
- queries: bfloat16 [16384, 3072], P(('seq', 'exp')), may hold values from -123 to 123
- keys: bfloat16 [16384, 512], P(('seq', 'exp')), may hold values from -6 to 6
- values: bfloat16 [16384, 512], P(('seq', 'exp')), may hold values from -9 to 9
- residual: bfloat16 [16384, 6144], P(('seq', 'exp')), may hold values from -51 to 51
- proj_weight: bfloat16 [3072, 6144], P('seq', 'exp'), may hold values from -0.109375 to 0.109375
- norm_gain: bfloat16 [6144], replicated, may hold values from 0.099609375 to 1.8984375
- router: bfloat16 [6144, 8], replicated, may hold values from -0.078125 to 0.078125
- expert_ids: int32 [16384, 2], P(('seq', 'exp')), may hold values from 0 to 7, all different within a row; in each aligned block of 128 rows (0 to 127, 128 to 255, ...) at most 33 rows name the same one
- u_gate_up: bfloat16 [16, 3072, 1024], P('exp'), may hold values from -0.078125 to 0.078125
- v_gate_up: bfloat16 [16, 2, 512, 4096], P('exp'), may hold values from -0.25 to 0.25
- u_down: bfloat16 [16, 4096, 512], P('exp'), may hold values from -0.0625 to 0.0625
- v_down: bfloat16 [16, 512, 3072], P('exp'), may hold values from -0.25 to 0.25
Outputs:
- layer_out: bfloat16 [16384, 6144], P(('seq', 'exp'))
The draws below stay inside these ranges and needn't reach their ends.
Inputs may be any that keep to these rules, and one draw needn't show every extreme that they name: `expert_ids`: the two experts of a token differ. Among the tokens of one device no expert is named more than 33 times, and in some devices' tokens some expert is named exactly 33 times.
All inputs are finite; a program needn't handle non-finite values.
Results may differ from the reference program's by a relative error of at most 0.02.
Values may be sent and summed in bfloat16 or wider, within the bound.
A program may use at most 192 MiB of HBM per device.

```python
import math
import jax
import jax.numpy as jnp
import numpy as np
from jax import lax

D = 6144
HEADS = 24
KV_HEADS = 4
HEAD_DIM = 128
EXPERTS = 8
TOP = 2
RANK = 512
FF = 8192
TOK_DEV = 128
CAP = 33
PIECES = 2
TOKENS = 16384


def draw_queries(key, part):
    noise_draw = jax.random.normal(jax.random.fold_in(key, 902), (TOKENS, HEADS, HEAD_DIM), jnp.float32)
    noise_draw = jnp.clip(noise_draw, -6.0, 6.0)
    return noise_draw.reshape(TOKENS, HEADS * HEAD_DIM).astype(jnp.bfloat16)


def draw_keys(key, part):
    noise_draw = jax.random.normal(jax.random.fold_in(key, 903), (TOKENS, KV_HEADS, HEAD_DIM), jnp.float32)
    noise_draw = jnp.clip(noise_draw, -6.0, 6.0)
    return noise_draw.reshape(TOKENS, KV_HEADS * HEAD_DIM).astype(jnp.bfloat16)


def draw_values(key, part):
    noise_draw = jax.random.normal(jax.random.fold_in(key, 904), (TOKENS, KV_HEADS * HEAD_DIM), jnp.float32)
    noise_draw = jnp.clip(noise_draw, -6.0, 6.0)
    levels = jax.random.normal(jax.random.fold_in(key, 905), (TOKENS // 256, KV_HEADS * HEAD_DIM), jnp.float32)
    levels = jnp.clip(levels, -3.0, 3.0)
    level_rows = jnp.repeat(levels, 256, axis=0)
    return (noise_draw + level_rows).astype(jnp.bfloat16)


def draw_residual(key, part):
    noise_draw = jax.random.normal(jax.random.fold_in(key, 907), (TOKENS, D), jnp.float32)
    noise_draw = jnp.clip(noise_draw, -4.0, 4.0)
    return noise_draw.astype(jnp.bfloat16)


def block_levels(own_key, dims, shards, least, top_value):
    gain = 1.0
    for dim, parts in shards:
        heights = jax.random.uniform(jax.random.fold_in(jax.random.fold_in(own_key, 6), dim), (parts,), jnp.float32, least / len(shards), top_value / len(shards))
        gain = gain * jnp.repeat(jnp.exp(heights), dims[dim] // parts).reshape((-1,) + (1,) * (len(dims) - 1 - dim))
    return gain


def assign_block(own_key, own, number, rows, number_of, top, limit, slope):
    ranking = jax.random.permutation(own_key, number_of)
    heavy_load, ordinary = load_shares(number_of, rows * top, limit, slope, True), load_shares(number_of, rows * top, limit, slope, False)
    places = jnp.arange(number_of)

    def named(lengths, turn):
        used = int((lengths > 0).sum())
        fixed = max(1, used // 4)
        passed = fixed + (places - fixed + turn * (used - fixed)) % max(1, number_of - fixed)
        return jnp.zeros((number_of,), jnp.int32).at[ranking[jnp.where(places < fixed, places, passed)]].set(jnp.asarray(lengths, jnp.int32))

    lengths = jnp.where(number % 4 == 0, named(heavy_load, number // 4), named(ordinary, number - number // 4 - 1))
    mixed = jax.random.permutation(jax.random.fold_in(own, 3), number_of)
    giver, sink = mixed[0:number_of // 2 * 2:2], mixed[1:number_of // 2 * 2:2]
    slack = jnp.minimum(lengths[giver] - 1, limit - lengths[sink]) // 2
    slack = jnp.where((giver == ranking[0]) | (sink == ranking[0]) | (lengths[sink] == 0), 0, jnp.maximum(slack, 0))
    passed = jax.random.randint(jax.random.fold_in(own, 4), (number_of // 2,), 0, 1 << 20) % (slack + 1)
    lengths = lengths.at[giver].add(-passed).at[sink].add(passed)
    items = jnp.searchsorted(jnp.cumsum(lengths), jnp.arange(rows * top), side="right").astype(jnp.int32)
    grid = items.reshape(top, rows).T
    grid = grid[jax.random.permutation(jax.random.fold_in(own, 1), rows)]
    turn = jax.random.randint(jax.random.fold_in(own, 2), (rows, 1), 0, top)
    return jnp.take_along_axis(grid, (jnp.arange(top)[None, :] + turn) % top, axis=1)


def load_shares(amount, total, most, slope, full):
    weights = [(1 << 20) // math.isqrt(rank ** slope) + 1 for rank in range(1, amount + 1)]
    largest = most if full else min(most, max(-(-total // amount), total * weights[0] // sum(weights)))
    least = 1 if total - largest >= amount - 1 else 0
    given, surplus = [largest] + [least] * (amount - 1), total - largest - least * (amount - 1)
    while surplus > 0:
        movable = [i for i in range(1, amount) if given[i] < largest] or [i for i in range(1, amount) if given[i] < most]
        whole, left = sum([weights[i] for i in movable]), surplus
        for i in movable:
            more = min(most - given[i], max(1, left * weights[i] // whole), surplus)
            given[i] = given[i] + more
            surplus = surplus - more
    return np.array(given)


def normal_values(key, shape, scale, bound, split=(), kind=jnp.bfloat16):
    factor_of = block_levels(key, shape, split, -0.22, 0.18) if split else 1.0
    drawn = jax.random.normal(key, shape, jnp.float32) * scale * factor_of
    return jnp.minimum(jnp.maximum(drawn, -bound), bound).astype(kind)


def setup_inputs(seed: int = 0) -> dict:
    streams_of = jax.random.split(jax.random.key(seed), 13)
    queries = draw_queries(jax.random.fold_in(streams_of[12], 71), 0)
    keys = draw_keys(jax.random.fold_in(streams_of[12], 71), 0)
    values = draw_values(jax.random.fold_in(streams_of[12], 71), 0)
    residual = draw_residual(jax.random.fold_in(streams_of[12], 71), 0)
    proj_weight = normal_values(streams_of[4], (HEADS * HEAD_DIM, D), (HEADS * HEAD_DIM) ** -0.5, 0.109375, ((0, 8), (1, 16)))
    norm_gain = jnp.clip(1.0 + 0.18 * jax.random.normal(streams_of[5], (D,), jnp.float32), 0.099609375, 1.8984375).astype(jnp.bfloat16)
    router = normal_values(streams_of[6], (D, EXPERTS), D ** -0.5, 0.078125)
    expert_ids_keys = jax.random.split(jax.random.fold_in(streams_of[7], 1), TOKENS // TOK_DEV)
    expert_ids_turns = jax.random.permutation(jax.random.fold_in(streams_of[7], 3), TOKENS // TOK_DEV)
    expert_ids = jax.vmap(lambda own, number: assign_block(jax.random.fold_in(streams_of[7], 2), own, number, TOK_DEV, EXPERTS, TOP, CAP, 2))(expert_ids_keys, expert_ids_turns).reshape((TOKENS, TOP))
    u_gate_up = normal_values(streams_of[8], (EXPERTS * PIECES, D // PIECES, 2 * RANK), D ** -0.5, 0.078125, ((0, 16),))
    v_gate_up = normal_values(streams_of[9], (EXPERTS * PIECES, 2, RANK, FF // PIECES), RANK ** -0.5, 0.25, ((0, 16),))
    u_down = normal_values(streams_of[10], (EXPERTS * PIECES, FF // PIECES, RANK), FF ** -0.5, 0.0625, ((0, 16),))
    v_down = normal_values(streams_of[11], (EXPERTS * PIECES, RANK, D // PIECES), RANK ** -0.5, 0.25, ((0, 16),))
    return {"queries": queries, "keys": keys, "values": values, "residual": residual, "proj_weight": proj_weight, "norm_gain": norm_gain, "router": router, "expert_ids": expert_ids, "u_gate_up": u_gate_up, "v_gate_up": v_gate_up, "u_down": u_down, "v_down": v_down}


EPS = 1e-05

def causal_attention(queries, keys, values):
    tile_rows = min(1024, TOKENS)
    tile_count = TOKENS // tile_rows
    per_kv = HEADS // KV_HEADS
    query_tiles = queries.reshape(tile_count, tile_rows, KV_HEADS, per_kv, HEAD_DIM)
    key_tiles = keys.reshape(tile_count, tile_rows, KV_HEADS, HEAD_DIM)
    value_tiles = values.reshape(tile_count, tile_rows, KV_HEADS, HEAD_DIM)
    score_scale = HEAD_DIM ** (-0.5)
    offsets = jnp.arange(tile_rows, dtype=jnp.int32)

    def one_tile(tile_index):
        query_block = lax.dynamic_index_in_dim(query_tiles, tile_index, 0, keepdims=False).astype(jnp.float32)
        query_pos = tile_index * tile_rows + offsets

        def scores_of(key_index):
            key_block = lax.dynamic_index_in_dim(key_tiles, key_index, 0, keepdims=False).astype(jnp.float32)
            scores = jnp.einsum('qhjd,khd->hjqk', query_block, key_block) * score_scale
            key_pos = key_index * tile_rows + offsets
            allowed = key_pos[None, :] <= query_pos[:, None]
            return jnp.where(allowed[None, None], scores, -jnp.inf)

        def max_step(key_index, row_max):
            return jnp.maximum(row_max, lax.optimization_barrier(jnp.max(scores_of(key_index), axis=-1)))
        start_max = jnp.full((KV_HEADS, per_kv, tile_rows), -jnp.inf, jnp.float32)
        row_max = lax.fori_loop(jnp.int32(0), tile_index + 1, max_step, start_max)

        def sum_step(key_index, carried):
            row_sum, weighted = carried
            exp_terms = jnp.exp(scores_of(key_index) - row_max[..., None])
            rounded = lax.optimization_barrier(exp_terms.astype(jnp.bfloat16)).astype(jnp.float32)
            value_block = lax.dynamic_index_in_dim(value_tiles, key_index, 0, keepdims=False).astype(jnp.float32)
            row_sum = row_sum + lax.optimization_barrier(jnp.sum(exp_terms, axis=-1))
            weighted = weighted + jnp.einsum('hjqk,khd->hjqd', rounded, value_block)
            return (row_sum, weighted)
        start_sum = jnp.zeros((KV_HEADS, per_kv, tile_rows), jnp.float32)
        start_acc = jnp.zeros((KV_HEADS, per_kv, tile_rows, HEAD_DIM), jnp.float32)
        row_sum, weighted = lax.fori_loop(jnp.int32(0), tile_index + 1, sum_step, (start_sum, start_acc))
        result = weighted / row_sum[..., None]
        return jnp.transpose(result, (2, 0, 1, 3)).reshape(tile_rows, HEADS * HEAD_DIM)
    outputs = lax.map(one_tile, jnp.arange(tile_count, dtype=jnp.int32))
    return outputs.reshape(TOKENS, HEADS * HEAD_DIM).astype(jnp.bfloat16)

def expert_stack(u_gate_up, v_gate_up, u_down, v_down):
    first_in = u_gate_up.reshape(EXPERTS, D, 2 * RANK)
    second_in = jnp.transpose(v_gate_up.reshape(EXPERTS, PIECES, 2, RANK, FF // PIECES), (0, 2, 3, 1, 4))
    second_in = second_in.reshape(EXPERTS, 2, RANK, FF)
    first_out = u_down.reshape(EXPERTS, FF, RANK)
    second_out = jnp.transpose(v_down.reshape(EXPERTS, PIECES, RANK, D // PIECES), (0, 2, 1, 3))
    second_out = second_out.reshape(EXPERTS, RANK, D)
    return (first_in, second_in, first_out, second_out)

def reference(queries, keys, values, residual, proj_weight, norm_gain, router, expert_ids, u_gate_up, v_gate_up, u_down, v_down):
    attended = causal_attention(queries, keys, values)
    attn_update = jnp.dot(attended, proj_weight, preferred_element_type=jnp.float32).astype(jnp.bfloat16)
    stream = residual.astype(jnp.float32) + attn_update.astype(jnp.float32)
    mean_sq = lax.optimization_barrier(jnp.mean(stream * stream, axis=-1, keepdims=True))
    normed = (stream * lax.rsqrt(mean_sq + EPS) * norm_gain.astype(jnp.float32)).astype(jnp.bfloat16)
    logits = jnp.dot(normed, router, preferred_element_type=jnp.float32)
    expert_range = jnp.arange(EXPERTS, dtype=jnp.int32)
    picked = (expert_ids[:, :, None] == expert_range[None, None, :]).astype(jnp.float32)
    chosen = lax.optimization_barrier(jnp.sum(picked * logits[:, None, :], axis=-1))
    mix_first = jax.nn.sigmoid(chosen[:, 0] - chosen[:, 1])
    mix_second = jax.nn.sigmoid(chosen[:, 1] - chosen[:, 0])
    mix_weight = jnp.stack([mix_first, mix_second], axis=1)
    block_count = TOKENS // TOK_DEV
    normed_blocks = normed.reshape(block_count, TOK_DEV, D).astype(jnp.float32)
    ids_blocks = expert_ids.reshape(block_count, TOK_DEV * 2)
    weight_blocks = mix_weight.reshape(block_count, TOK_DEV, 2)
    slot_range = jnp.arange(CAP, dtype=jnp.int32)
    first_in, second_in, first_out, second_out = expert_stack(u_gate_up, v_gate_up, u_down, v_down)

    def one_expert(carried, expert_index):
        member = (ids_blocks == expert_index).astype(jnp.int32)
        slot_of = jnp.cumsum(member, axis=1) - 1
        placed = (member[..., None] * (slot_of[..., None] == slot_range).astype(jnp.int32)).astype(jnp.float32)
        placed_tok = placed.reshape(block_count, TOK_DEV, 2, CAP)
        select = lax.optimization_barrier(jnp.sum(placed_tok, axis=2))
        rows_in = jnp.einsum('btc,btd->bcd', select, normed_blocks).astype(jnp.bfloat16)
        rows_in = rows_in.reshape(block_count * CAP, D)
        w_first = lax.dynamic_index_in_dim(first_in, expert_index, 0, keepdims=False)
        w_middle = lax.dynamic_index_in_dim(second_in, expert_index, 0, keepdims=False)
        w_down = lax.dynamic_index_in_dim(first_out, expert_index, 0, keepdims=False)
        w_last = lax.dynamic_index_in_dim(second_out, expert_index, 0, keepdims=False)
        rank_in = jnp.dot(rows_in, w_first, preferred_element_type=jnp.float32).astype(jnp.bfloat16)
        gate_part = jnp.dot(rank_in[:, :RANK], w_middle[0], preferred_element_type=jnp.float32)
        up_part = jnp.dot(rank_in[:, RANK:], w_middle[1], preferred_element_type=jnp.float32)
        hidden = (jax.nn.silu(gate_part) * up_part).astype(jnp.bfloat16)
        rank_down = jnp.dot(hidden, w_down, preferred_element_type=jnp.float32).astype(jnp.bfloat16)
        out_rows = jnp.dot(rank_down, w_last, preferred_element_type=jnp.float32).astype(jnp.bfloat16)
        back_rows = out_rows.astype(jnp.float32).reshape(block_count, CAP, D)
        weights_tok = jnp.einsum('btsc,bts->btc', placed_tok, weight_blocks)
        carried = carried + jnp.einsum('btc,bcd->btd', weights_tok, back_rows)
        return (carried, None)
    start_mix = jnp.zeros((block_count, TOK_DEV, D), jnp.float32)
    mixture, unused = lax.scan(one_expert, start_mix, jnp.arange(EXPERTS, dtype=jnp.int32))
    return (stream + mixture.reshape(TOKENS, D)).astype(jnp.bfloat16)
```

```python
import jax
import jax.numpy as jnp
from jax import lax
from jax.experimental import pallas as pl
from jax.experimental.pallas import tpu as pltpu
from jax.sharding import Mesh, PartitionSpec as P

D = 6144
PER_KV = 6
HEAD_DIM = 128
WIDTH = PER_KV * HEAD_DIM
EXPERTS = 8
RANK = 512
TOK_DEV = 128
CAP = 33
MAIN = 32
EPS = 1e-05
AXES = ("zh", "x", "zl", "y", "c")
BLOCKS = ("zh", "x", "zl", "c")
PLANE = ("zh", "x", "zl")
EXP = ("zl", "y", "c")
SCORE_SCALE = HEAD_DIM ** (-0.5) * 1.4426950408889634
HALF = 1024
TILE = 256
MESH = pl.DeviceIdType.MESH
VM = pl.BlockSpec(memory_space=pltpu.VMEM)
SM = pl.BlockSpec(memory_space=pltpu.SMEM)
COPIES = 85


def exchange_kernel(q_ref, k_ref, v_ref, qo_ref, ko_ref, vo_ref, sends, recvs, local):
    zh, x, zl, y, c = [lax.axis_index(name) for name in AXES]
    z = zh * 2 + zl

    def device(z_, x_, y_, c_):
        return (z_ // 2, x_, z_ % 2, y_, c_)

    def ring(at, step):
        return lax.rem(at + step + 4, 4)

    y_peers = [device(z, x, ring(y, d), c) for d in (1, 2, 3)]
    far_peers = [device(3 - z, 3 - x, ring(y, d), c) for d in (0, 1, 2, 3)]
    partner = device(z, x, y, 1 - c)
    x_up, x_down = device(z, ring(x, 1), y, c), device(z, ring(x, -1), y, c)
    z_up, z_down = device(ring(z, 1), x, y, c), device(ring(z, -1), x, y, c)
    everyone = y_peers + far_peers + [partner, x_up, x_down, z_up, z_down]
    barrier = pltpu.get_barrier_semaphore()
    for peer in everyone:
        pl.semaphore_signal(barrier, inc=1, device_id=peer, device_id_type=MESH)
    pl.semaphore_wait(barrier, len(everyone))

    started = []

    def send(source, target, peer):
        at = len(started)
        copy = pltpu.make_async_remote_copy(
            src_ref=source,
            dst_ref=target,
            send_sem=sends.at[at],
            recv_sem=recvs.at[at],
            device_id=peer,
            device_id_type=MESH,
        )
        copy.start()
        started.append(copy)
        return copy

    def columns(ref, rows, head, width):
        return ref.at[rows, pl.ds(pl.multiple_of(head * width, 128), width)]

    every = slice(0, TOK_DEV)
    own_rows = pl.ds(pl.multiple_of(y * TOK_DEV, TOK_DEV), TOK_DEV)
    q_rows = pl.ds(pl.multiple_of(y * 64, 64), 64)
    k_in, v_in, q_in = [], [], []
    for into, ref, out in ((k_in, k_ref, ko_ref), (v_in, v_ref, vo_ref)):
        for d, peer in zip((1, 2, 3), y_peers):
            into.append(
                send(
                    columns(ref, every, ring(y, d), HEAD_DIM),
                    out.at[z, x, c, own_rows],
                    peer,
                )
            )
    for d, peer in zip((1, 2, 3), y_peers):
        q_in.append(
            send(columns(q_ref, slice(0, 64), ring(y, d), WIDTH), qo_ref.at[0, q_rows], peer)
        )
    for d, peer in zip((0, 1, 2, 3), far_peers):
        q_in.append(
            send(columns(q_ref, slice(64, 128), ring(y, d), WIDTH), qo_ref.at[1, q_rows], peer)
        )
    own = [
        (columns(k_ref, every, y, HEAD_DIM), ko_ref.at[z, x, c, own_rows]),
        (columns(v_ref, every, y, HEAD_DIM), vo_ref.at[z, x, c, own_rows]),
        (columns(q_ref, slice(0, 64), y, WIDTH), qo_ref.at[0, q_rows]),
    ]
    own = [
        pltpu.make_async_copy(source, target, local.at[at])
        for at, (source, target) in enumerate(own)
    ]
    for copy in own:
        copy.start()

    class Color:
        def __init__(self, ref, x_first):
            self.ref, self.x_first = ref, x_first
            self.first, self.second = (x, z) if x_first else (z, x)
            self.f_up, self.f_down = (x_up, x_down) if x_first else (z_up, z_down)
            self.s_up, self.s_down = (z_up, z_down) if x_first else (x_up, x_down)
            self.across = []
            self.spread = []

        def chunk(self, f, s):
            f, s = ring(self.first, f), ring(self.second, s)
            z_, x_ = (s, f) if self.x_first else (f, s)
            return self.ref.at[z_, x_, c]

        def part(self, f, s, number):
            f, s = ring(self.first, f), ring(self.second, s)
            z_, x_ = (s, f) if self.x_first else (f, s)
            return self.ref.at[z_, x_, c, slice(number * 256, number * 256 + 256)]

        def pass_on(self, f, s):
            piece = self.chunk(f, s)
            self.across.append(send(piece, piece, partner))

        def second_way(self, f):
            piece = self.chunk(f, 0)
            up, down = send(piece, piece, self.s_up), send(piece, piece, self.s_down)
            self.spread.append((f, up, down))

        def begin(self):
            piece = self.chunk(0, 0)
            self.up, self.down = send(piece, piece, self.f_up), send(piece, piece, self.f_down)
            self.second_way(0)
            self.pass_on(0, 0)

        def forward_first(self):
            self.up.wait_recv()
            piece = self.part(-1, 0, 0)
            self.up_part = send(piece, piece, self.f_up)
            self.down.wait_recv()
            piece = self.part(1, 0, 1)
            self.down_part = send(piece, piece, self.f_down)
            for f in (-1, 1):
                self.second_way(f)
                self.pass_on(f, 0)

        def finish_first(self):
            self.up_part.wait_recv()
            self.down_part.wait_recv()
            self.second_way(2)
            self.pass_on(2, 0)

        def forward_second(self, at):
            f, up, down = self.spread[at]
            up.wait_recv()
            piece = self.part(f, -1, 0)
            up_part = send(piece, piece, self.s_up)
            down.wait_recv()
            piece = self.part(f, 1, 1)
            down_part = send(piece, piece, self.s_down)
            self.spread[at] = (f, up_part, down_part)
            self.pass_on(f, -1)
            self.pass_on(f, 1)

        def finish_second(self, at):
            f, up_part, down_part = self.spread[at]
            up_part.wait_recv()
            down_part.wait_recv()
            self.pass_on(f, 2)

    key_color, value_color = Color(ko_ref, True), Color(vo_ref, False)
    colors = (key_color, value_color)
    own[0].wait()
    for copy in k_in:
        copy.wait_recv()
    key_color.begin()
    own[1].wait()
    for copy in v_in:
        copy.wait_recv()
    value_color.begin()
    for color in colors:
        color.forward_first()
    for color in colors:
        color.finish_first()
    for at in range(4):
        for color in colors:
            color.forward_second(at)
    for at in range(4):
        for color in colors:
            color.finish_second(at)
    own[2].wait()
    for copy in q_in:
        copy.wait_recv()
    for color in colors:
        for copy in color.across:
            copy.wait_recv()
    for copy in started:
        copy.wait_send()
    assert len(started) == COPIES


def exchange(queries, keys, values):
    kv = jax.ShapeDtypeStruct((4, 4, 2, 512, HEAD_DIM), jnp.bfloat16)
    return pl.pallas_call(
        exchange_kernel,
        out_shape=(jax.ShapeDtypeStruct((2, TILE, WIDTH), jnp.bfloat16), kv, kv),
        in_specs=[VM, VM, VM],
        out_specs=(VM, VM, VM),
        scratch_shapes=[
            pltpu.SemaphoreType.DMA((COPIES,)),
            pltpu.SemaphoreType.DMA((COPIES,)),
            pltpu.SemaphoreType.DMA((3,)),
        ],
        compiler_params=pltpu.CompilerParams(collective_id=1, has_side_effects=True),
        cost_estimate=pl.CostEstimate(
            flops=30_000_000_000, bytes_accessed=12 << 20, transcendentals=0
        ),
        name="exchange",
    )(queries, keys, values)


def attend_step(q_ref, slot, keys, values, first_row, m_ref, acc_ref):
    ones = jnp.ones((HALF, HEAD_DIM), jnp.bfloat16)
    value_ones = jnp.concatenate([values, ones], axis=1)
    if first_row is not None:
        row = lax.broadcasted_iota(jnp.int32, (TILE, HALF), 0)
        row = (row // 64) * 256 + row % 64 + first_row
        col = lax.broadcasted_iota(jnp.int32, (TILE, HALF), 1)
        col = (col % 512) // 128 * 256 + (col // 512) * 128 + col % 128
        allowed = col <= row
    for head in range(PER_KV):
        q = q_ref[slot, :, head * HEAD_DIM : (head + 1) * HEAD_DIM]
        s = lax.dot_general(
            q, keys, (((1,), (1,)), ((), ())), preferred_element_type=jnp.float32
        )
        s = s * SCORE_SCALE
        if first_row is not None:
            s = jnp.where(allowed, s, -1e30)
        m_prev = m_ref[slot, head]
        m_new = jnp.maximum(m_prev, jnp.max(s, axis=1, keepdims=True))
        parts = [
            jnp.exp2(s[:, at : at + HEAD_DIM] - m_new).astype(jnp.bfloat16)
            for at in range(0, HALF, HEAD_DIM)
        ]
        weights = jnp.concatenate(parts, axis=1)
        fade = jnp.exp2(m_prev - m_new)
        fade = jnp.concatenate([fade, fade], axis=1)
        update = jnp.dot(weights, value_ones, preferred_element_type=jnp.float32)
        acc_ref[slot, head] = acc_ref[slot, head] * fade + update
        m_ref[slot, head] = m_new


def attend_kernel(where_ref, q_ref, k_ref, v_ref, o_ref, m_ref, acc_ref):
    m_ref[...] = jnp.full(m_ref.shape, -1e30, jnp.float32)
    acc_ref[...] = jnp.zeros(acc_ref.shape, jnp.float32)

    def block(slot, number, first_row):
        z, x = number // 8 * 2 + number % 2, number // 2 % 4
        keys = k_ref[z, x].reshape(HALF, HEAD_DIM)
        values = v_ref[z, x].reshape(HALF, HEAD_DIM)
        attend_step(q_ref, slot, keys, values, first_row, m_ref, acc_ref)

    for slot in range(2):
        last = where_ref[slot]

        def step(number, carry, slot=slot):
            block(slot, number, None)
            return carry

        lax.fori_loop(0, last, step, 0)
        block(slot, last, where_ref[2] + slot * 64)
        for head in range(PER_KV):
            at = head * HEAD_DIM
            o_ref[slot, :, at : at + HEAD_DIM] = (
                acc_ref[slot, head, :, :HEAD_DIM] / acc_ref[slot, head, :, HEAD_DIM:]
            ).astype(jnp.bfloat16)


def attend(where, q, k, v):
    return pl.pallas_call(
        attend_kernel,
        out_shape=jax.ShapeDtypeStruct((2, TILE, WIDTH), jnp.bfloat16),
        in_specs=[SM, VM, VM, VM],
        out_specs=VM,
        scratch_shapes=[
            pltpu.VMEM((2, PER_KV, TILE, HEAD_DIM), jnp.float32),
            pltpu.VMEM((2, PER_KV, TILE, 2 * HEAD_DIM), jnp.float32),
        ],
        cost_estimate=pl.CostEstimate(
            flops=17 * PER_KV * TILE * HALF * HEAD_DIM * 4,
            bytes_accessed=12 << 20,
            transcendentals=17 * PER_KV * TILE * HALF,
        ),
        name="attend",
    )(where, q, k, v)


def project_kernel(o_ref, w_ref, out_ref):
    total = None
    for s in range(8):
        at = s % 2 * 384
        term = jnp.dot(
            o_ref[s // 2, :, at : at + 384], w_ref[s, 0], preferred_element_type=jnp.float32
        )
        total = term if total is None else total + term
    total = total.astype(jnp.bfloat16)
    for half in range(2):
        for y in range(4):
            at = half * 256 + y * 64
            out_ref[y, 0, half * 64 : half * 64 + 64, :] = total[at : at + 64]


def project(attended, weight):
    return pl.pallas_call(
        project_kernel,
        grid=(4,),
        out_shape=jax.ShapeDtypeStruct((4, 4, TOK_DEV, 384), jnp.bfloat16),
        in_specs=[
            pl.BlockSpec((4, 512, WIDTH), lambda q: (0, 0, 0)),
            pl.BlockSpec((8, 1, 384, 384), lambda q: (0, q, 0, 0)),
        ],
        out_specs=pl.BlockSpec((4, 1, TOK_DEV, 384), lambda q: (0, q, 0, 0)),
        cost_estimate=pl.CostEstimate(
            flops=2 * 512 * 3072 * 1536, bytes_accessed=14 << 20, transcendentals=0
        ),
        name="project",
    )(attended, weight)


def update_at(update_ref, number):
    return update_ref[number // 2 % 4, number // 8 * 2 + number % 2].astype(jnp.float32)


def route_kernel(
    update_ref, residual_ref, gain_ref, router_ref, ids_ref,
    main_ref, extra_ref, hi_ref, lo_ref, stream_ref, normed_ref,
):
    square = jnp.zeros((TOK_DEV, 1), jnp.float32)
    for number in range(16):
        cols = slice(number * 384, number * 384 + 384)
        stream = residual_ref[:, cols].astype(jnp.float32) + update_at(update_ref, number)
        stream_ref[:, cols] = stream
        square = square + jnp.sum(stream * stream, axis=1, keepdims=True)
    scale = lax.rsqrt(square * (1.0 / D) + EPS)
    logits = jnp.zeros((TOK_DEV, EXPERTS), jnp.float32)
    for number in range(16):
        cols = slice(number * 384, number * 384 + 384)
        normed = stream_ref[:, cols] * scale * gain_ref[:, cols].astype(jnp.float32)
        normed = normed.astype(jnp.bfloat16)
        normed_ref[:, cols] = normed
        logits = logits + jnp.dot(
            normed, router_ref[cols, :], preferred_element_type=jnp.float32
        )
    first, second = ids_ref[:, 0:1], ids_ref[:, 1:2]
    expert = lax.broadcasted_iota(jnp.int32, (TOK_DEV, EXPERTS), 1)
    is_first = (expert == first).astype(jnp.float32)
    is_second = (expert == second).astype(jnp.float32)
    row = lax.broadcasted_iota(jnp.int32, (TOK_DEV, TOK_DEV), 0)
    col = lax.broadcasted_iota(jnp.int32, (TOK_DEV, TOK_DEV), 1)
    before = (col < row).astype(jnp.float32)
    slot = jnp.dot(before, is_first + is_second, preferred_element_type=jnp.float32)

    def pick(table, values):
        return jnp.sum(table * values, axis=1, keepdims=True)

    first_slot = pick(is_first, slot).astype(jnp.int32)
    second_slot = pick(is_second, slot).astype(jnp.int32)
    first_logit, second_logit = pick(is_first, logits), pick(is_second, logits)
    mix_first = 1.0 / (1.0 + jnp.exp(second_logit - first_logit))
    mix_second = 1.0 / (1.0 + jnp.exp(first_logit - second_logit))
    lane = lax.broadcasted_iota(jnp.int32, (TOK_DEV, 384), 1)
    lane_expert = jnp.where(lane < 256, lane // MAIN, lane - 256)
    lane_slot = jnp.where(lane < 256, lane % MAIN, MAIN)
    in_first = (lane_expert == first) & (lane_slot == first_slot)
    in_second = (lane_expert == second) & (lane_slot == second_slot)
    combine = jnp.where(in_first, mix_first, jnp.where(in_second, mix_second, 0.0))
    high = combine.astype(jnp.bfloat16)
    hi_ref[...] = high
    lo_ref[...] = (combine - high.astype(jnp.float32)).astype(jnp.bfloat16)
    place = jnp.where(in_first | in_second, 1.0, 0.0).T.astype(jnp.bfloat16)
    for number in range(8):
        cols = slice(number * 768, number * 768 + 768)
        rows = jnp.dot(place, normed_ref[:, cols], preferred_element_type=jnp.float32)
        rows = rows.astype(jnp.bfloat16)
        piece, at = number // 4, number % 4 * 768
        for k in range(EXPERTS):
            main_ref[2 * k + piece, :, at : at + 768] = rows[k * MAIN : k * MAIN + MAIN]
        extra_ref[:, cols] = rows[256:264]


def route(update, residual, gain, router, ids):
    weights = jax.ShapeDtypeStruct((TOK_DEV, 384), jnp.bfloat16)
    return pl.pallas_call(
        route_kernel,
        out_shape=(
            jax.ShapeDtypeStruct((16, MAIN, D // 2), jnp.bfloat16),
            jax.ShapeDtypeStruct((EXPERTS, D), jnp.bfloat16),
            weights,
            weights,
        ),
        in_specs=[VM] * 5,
        out_specs=(VM,) * 4,
        scratch_shapes=[
            pltpu.VMEM((TOK_DEV, D), jnp.float32),
            pltpu.VMEM((TOK_DEV, D), jnp.bfloat16),
        ],
        cost_estimate=pl.CostEstimate(
            flops=2 * 384 * 128 * D, bytes_accessed=8 << 20, transcendentals=0
        ),
        name="route",
    )(update, residual, gain, router, ids)


def combine_kernel(
    update_ref, residual_ref, hi_ref, lo_ref, main_ref, extra_ref, out_ref
):
    for number in range(16):
        cols = slice(number * 384, number * 384 + 384)
        piece, at = number // 8, number % 8 * 384
        rows = main_ref[:, piece, :, at : at + 384].reshape(256, 384)
        last = extra_ref[:, cols]
        total = residual_ref[:, cols].astype(jnp.float32) + update_at(update_ref, number)
        for weight_ref in (hi_ref, lo_ref):
            total = total + jnp.dot(
                weight_ref[:, :256], rows, preferred_element_type=jnp.float32
            )
            total = total + jnp.dot(
                weight_ref[:, 256 : 256 + EXPERTS], last, preferred_element_type=jnp.float32
            )
        out_ref[:, cols] = total.astype(jnp.bfloat16)


def combine(update, residual, hi, lo, main, extra):
    return pl.pallas_call(
        combine_kernel,
        out_shape=jax.ShapeDtypeStruct((TOK_DEV, D), jnp.bfloat16),
        in_specs=[VM] * 6,
        out_specs=VM,
        cost_estimate=pl.CostEstimate(
            flops=4 * 256 * 128 * D, bytes_accessed=8 << 20, transcendentals=0
        ),
        name="combine",
    )(update, residual, hi, lo, main, extra)


def per_device(
    queries,
    keys,
    values,
    residual,
    proj_weight,
    norm_gain,
    router,
    expert_ids,
    u_gate_up,
    v_gate_up,
    u_down,
    v_down,
):
    block = lax.axis_index(PLANE)
    where = jnp.stack([block, 15 - block, lax.axis_index("c") * TOK_DEV]).astype(jnp.int32)
    weight = lax.all_gather(proj_weight, BLOCKS, axis=0, tiled=True).reshape(8, 4, 384, 384)
    q_pair, k_all, v_all = exchange(queries, keys, values)
    attended = attend(where, q_pair, k_all, v_all)
    attended, weight = lax.optimization_barrier((attended, weight))
    back = lax.ppermute(attended[1], PLANE, [(i, 15 - i) for i in range(16)])
    attended = jnp.concatenate([attended[0], back], axis=0)
    attended = lax.all_gather(attended, "y", axis=0, tiled=True).reshape(4, 512, WIDTH)
    projected = project(attended, weight)
    update = lax.all_to_all(projected, "y", split_axis=0, concat_axis=0, tiled=True)
    main, extra, hi, lo = route(
        update, residual, norm_gain.reshape(1, D), router, expert_ids
    )

    def to_experts(main, extra):
        extra = extra.reshape(16, 8, 384)
        return tuple(
            lax.all_to_all(rows, EXP, split_axis=0, concat_axis=0, tiled=True)
            for rows in (main, extra)
        )

    main, extra = to_experts(main, extra)
    expert_rows = jnp.concatenate(
        [main.reshape(16 * MAIN, D // 2), extra.reshape(16, D // 2)], axis=0
    )
    flip = [(0, 1), (1, 0)]
    rank_sum = jnp.dot(expert_rows, u_gate_up[0], preferred_element_type=jnp.float32)
    rank_sum = rank_sum + lax.ppermute(rank_sum.astype(jnp.bfloat16), "c", flip).astype(
        jnp.float32
    )
    rank_in = rank_sum.astype(jnp.bfloat16)
    gate_part = jnp.dot(rank_in[:, :RANK], v_gate_up[0, 0], preferred_element_type=jnp.float32)
    up_part = jnp.dot(rank_in[:, RANK:], v_gate_up[0, 1], preferred_element_type=jnp.float32)
    hidden = (jax.nn.silu(gate_part) * up_part).astype(jnp.bfloat16)
    down_sum = jnp.dot(hidden, u_down[0], preferred_element_type=jnp.float32)
    down_sum = down_sum + lax.ppermute(down_sum.astype(jnp.bfloat16), "c", flip).astype(
        jnp.float32
    )
    rank_down = down_sum.astype(jnp.bfloat16)
    main = jnp.dot(rank_down[: 16 * MAIN], v_down[0], preferred_element_type=jnp.float32)
    extra = jnp.dot(rank_down[16 * MAIN :], v_down[0], preferred_element_type=jnp.float32)
    main, extra = to_experts(
        main.astype(jnp.bfloat16).reshape(16, MAIN, D // 2), extra.astype(jnp.bfloat16)
    )
    return combine(
        update,
        residual,
        hi,
        lo,
        main.reshape(EXPERTS, 2, MAIN, D // 2),
        extra.reshape(EXPERTS, D),
    )


def solution(mesh):
    fine = Mesh(mesh.devices.reshape(2, 4, 2, 4, 2), AXES)
    in_specs = (
        P(AXES, None),
        P(AXES, None),
        P(AXES, None),
        P(AXES, None),
        P(("zh", "x"), EXP),
        P(),
        P(),
        P(AXES, None),
        P(EXP, None, None),
        P(EXP, None, None, None),
        P(EXP, None, None),
        P(EXP, None, None),
    )
    return jax.shard_map(
        per_device, mesh=fine, in_specs=in_specs, out_specs=P(AXES, None), check_vma=False
    )
```
